256 devices in a mesh: blk: 128 (over y, x_hi, z, core), row: 2 (over x_lo).
Axes of the slice: x: 4 (x_hi: 2, x_lo: 2; x = x_hi * 2 + x_lo), y: 4, z: 8, core: 2. Of those that a mesh axis runs over, the one named last changes fastest.
Arguments:
- features: bfloat16 [12288, 16384], P('row', 'blk'), parts along dimension 0, may hold values from -6 to 6
- link_values: bfloat16 [8, 32, 16384], P(None, None, 'blk'), may hold values from -1 to 1
- link_columns: int32 [8, 32, 16384], P(None, None, 'blk'), may hold values from 0 to 255
- layer_bias: float32 [8, 16384], P(None, 'blk'), may hold values from -0.5 to 0.5
Outputs:
- outputs: bfloat16 [12288, 16384], P('row', 'blk'), parts along dimension 0
The draws below stay inside these ranges and needn't reach their ends.
There are 2 independent parts, one for each index of `row`. The reference program is written for one: setup_inputs(seed, part) draws one part's arguments, and reference() takes and returns one part's arrays. A program takes and returns all parts, laid end to end along the dimension named above; an argument that names none is the same for every part. Nothing has to cross between parts.
All inputs are finite; a program needn't handle non-finite values.
Results may differ from the reference program's by a relative error of at most 0.0072.
Values may be sent and summed in bfloat16 or wider, within the bound.
A program may use at most 64 MiB of HBM per device.

```python
import math
import jax
import jax.numpy as jnp

BLOCK = 128
FANIN = 32
LAYERS = 8
ROWS = 6144
NEURONS = 16384
N_BLK = 128


def dense_choice(key):
    block_count = NEURONS // BLOCK
    layer_keys = jax.random.split(jax.random.fold_in(key, 911), LAYERS)
    orders = jax.vmap(lambda single: jax.random.permutation(single, block_count))(layer_keys)
    chosen = orders < block_count // 4
    return jnp.repeat(chosen, BLOCK, axis=1)


def draw_layer_bias(key, part):
    chosen = dense_choice(key)
    drawn = jax.random.uniform(jax.random.fold_in(key, 17), (LAYERS, NEURONS), jnp.float32, -0.5, 0.5)
    lifted = jax.random.uniform(jax.random.fold_in(key, 23), (LAYERS, NEURONS), jnp.float32, 0.3, 0.5)
    return jnp.where(chosen, lifted, drawn).astype(jnp.float32)


def draw_link_values(key, part):
    chosen = dense_choice(key)
    spread = 1.0 / math.sqrt(FANIN // 2)
    limit = 1.0 / spread
    unscaled = jax.random.truncated_normal(jax.random.fold_in(key, 37), -limit, limit, (LAYERS, FANIN, NEURONS), jnp.float32)
    factor = jnp.where(chosen, 0.3, 1.0).astype(jnp.float32)[:, None, :]
    return (unscaled * spread * factor).astype(jnp.bfloat16)


def touch_ends(drawn, rng, least, largest):
    extent = drawn.shape
    spot = [jax.random.randint(jax.random.fold_in(rng, axis), (), 0, extent[axis]) for axis in range(len(extent))]
    drawn = drawn.at[tuple(spot)].set(least)
    longest = extent.index(max(extent))
    spot[longest] = (spot[longest] + 1) % extent[longest]
    return drawn.at[tuple(spot)].set(largest)


def levels(own_key, shape, pieces, smallest, top_value):
    loudness, own = 1.0, jax.random.fold_in(own_key, 6)
    for dim, blocks in pieces:
        draws = jnp.exp(jax.random.uniform(jax.random.fold_in(own, dim), (blocks,), jnp.float32, smallest / len(pieces), top_value / len(pieces)))
        loudness = loudness * jnp.repeat(draws, shape[dim] // blocks).reshape([-1 if axis == dim else 1 for axis in range(len(shape))])
    return loudness


def gaussian(rng, dims, deviation, bound, cuts=(), kind=jnp.bfloat16):
    result = jax.random.normal(rng, dims, jnp.float32) * deviation
    if len(cuts) > 0:
        result = levels(rng, dims, cuts, -0.22, 0.18) * result
    return jnp.clip(result, min=-bound, max=bound).astype(kind)


def setup_inputs(seed: int = 0, part: int = 0) -> dict:
    key_of = jax.random.split(jax.random.key(seed), 5)
    part_keys = jax.random.split(jax.random.fold_in(key_of[4], part), 5)
    features = gaussian(part_keys[0], (ROWS, NEURONS), 1.0, 6.0, ((1, 128),))
    link_values = draw_link_values(jax.random.fold_in(key_of[4], 71), part)
    link_columns = touch_ends(jax.random.randint(key_of[2], (LAYERS, FANIN, NEURONS), 0, 2 * BLOCK), jax.random.fold_in(key_of[2], 1), 0, (2 * BLOCK) - 1).astype(jnp.int32)
    layer_bias = draw_layer_bias(jax.random.fold_in(key_of[4], 71), part)
    return {"features": features, "link_values": link_values, "link_columns": link_columns, "layer_bias": layer_bias}


ceiling_value = 4.0


def dense_layer(values_layer, columns_layer):
    target = jnp.broadcast_to(jnp.arange(NEURONS, dtype=jnp.int32)[None, :], columns_layer.shape)
    summed = jnp.zeros((NEURONS, 2 * BLOCK), jnp.float32).at[target, columns_layer.astype(jnp.int32)].add(values_layer.astype(jnp.float32))
    weights = summed.astype(jnp.bfloat16).reshape(N_BLK, BLOCK, 2 * BLOCK)
    return jnp.transpose(weights, (0, 2, 1))


def reference(features, link_values, link_columns, layer_bias):
    bit_count = N_BLK.bit_length() - 1
    blocks = features.reshape(ROWS, N_BLK, BLOCK)
    owners = jnp.arange(N_BLK, dtype=jnp.int32)
    for layer_at in range(LAYERS):
        stride = 2 ** (layer_at % bit_count)
        weights = dense_layer(link_values[layer_at], link_columns[layer_at]).astype(jnp.float32)
        partner = blocks[:, jnp.bitwise_xor(owners, stride).astype(jnp.int32)]
        preact = jnp.einsum('rnk,nko->rno', blocks.astype(jnp.float32), weights[:, :BLOCK])
        preact = preact + jnp.einsum('rnk,nko->rno', partner.astype(jnp.float32), weights[:, BLOCK:])
        preact = preact + layer_bias[layer_at].reshape(N_BLK, BLOCK)[None, :, :]
        blocks = jnp.minimum(jnp.maximum(preact, 0.0), ceiling_value).astype(jnp.bfloat16)
    return blocks.reshape(ROWS, NEURONS)
```

```python
import functools

import jax
import jax.numpy as jnp
from jax import lax
from jax.experimental import pallas as pl
from jax.experimental.pallas import tpu as pltpu
from jax.sharding import PartitionSpec as P

MESH = pl.DeviceIdType.MESH
LAYERS = 8
CEILING = 4.0
CHUNKS = 8
GROUP = 8
MASKS = (1, 2, 4)


def bits(value):
    return [(value // 2**k) % 2 for k in range(3)]


def xor(value_bits, mask):
    total = 0
    for k in range(3):
        flip = (mask >> k) & 1 if isinstance(mask, int) else mask[k]
        total = total + ((value_bits[k] + flip) % 2) * 2**k
    return total


def dense(values, columns):
    fan_in, width = values.shape
    field = lax.broadcasted_iota(jnp.int32, (2 * width, width), 0).astype(jnp.float32)
    total = jnp.zeros((2 * width, width), jnp.float32)
    for link in range(fan_in):
        total = total + jnp.where(field == columns[link : link + 1, :], values[link : link + 1, :], 0.0)
    return total.astype(jnp.bfloat16)


def activate(preact):
    return jnp.minimum(jnp.maximum(preact, 0.0), CEILING).astype(jnp.bfloat16)


def three_layers(slots, weights, bias, first_layer):
    width = slots[0].shape[1]
    for step, mask in enumerate(MASKS):
        after = [None] * GROUP
        for low in range(GROUP):
            if low & mask:
                continue
            high = low | mask
            w_low, w_high = weights[low, step], weights[high, step]
            w_high = jnp.concatenate([w_high[width:], w_high[:width]], axis=0)
            row = first_layer + step
            b_pair = jnp.concatenate([bias[low, row : row + 1, :], bias[high, row : row + 1, :]], axis=1)
            pair = jnp.dot(
                jnp.concatenate([slots[low], slots[high]], axis=1),
                jnp.concatenate([w_low, w_high], axis=1),
                preferred_element_type=jnp.float32,
            )
            pair = activate(pair + b_pair)
            after[low], after[high] = pair[:, :width], pair[:, width:]
        slots = after
    return slots


def kernel(
    features, values, columns, bias, out,
    partner_in, act0, z_in, z_out, back, x_in, x_out, home, partner_home,
    own_columns, z_values, z_columns, z_bias, x_bias, w_end, w_z, w_x,
    pf_s, pf_r, zi_s, zi_r, zo_s, zo_r, xi_s, xi_r, xo_s, xo_r, pl_s, pl_r, w_s, w_r,
):
    chunks, _, piece, width = features.shape
    block = lax.axis_index("blk")
    core, z, u = block % 2, (block // 2) % GROUP, block // (2 * GROUP)
    zb, ub = bits(z), bits(u)
    partner = block + 1 - 2 * core
    z_of = [xor(zb, j) for j in range(GROUP)]
    u_of = [xor(ub, j) for j in range(GROUP)]
    z_peer = [(u * GROUP + z_of[j]) * 2 + core for j in range(GROUP)]
    u_peer = [(u_of[j] * GROUP + z) * 2 + core for j in range(GROUP)]

    def copy(src, dst, send, recv, peer):
        return pltpu.make_async_remote_copy(
            src_ref=src, dst_ref=dst, send_sem=send, recv_sem=recv, device_id={"blk": peer}, device_id_type=MESH
        )

    barrier = pltpu.get_barrier_semaphore()
    peers = [partner, *z_peer[1:], *u_peer[1:]]
    for peer in peers:
        pl.semaphore_signal(barrier, inc=1, device_id={"blk": peer}, device_id_type=MESH)
    own_columns[...] = columns[...].astype(jnp.float32).astype(jnp.bfloat16)
    z_values[0] = values[1:4]
    z_columns[0] = columns[1:4].astype(jnp.float32).astype(jnp.bfloat16)
    z_bias[0] = bias[...]
    x_bias[0] = bias[...]
    pl.semaphore_wait(barrier, len(peers))

    def partner_copy(c):
        return copy(features.at[c], partner_in.at[c], pf_s.at[c], pf_r.at[c], partner)

    partner_copy(0).start()
    for j in range(1, GROUP):
        copy(bias, z_bias.at[j], w_s.at[0], w_r.at[0], z_peer[j]).start()
        copy(values.at[1:4], z_values.at[j], w_s.at[1], w_r.at[1], z_peer[j]).start()
        copy(own_columns.at[1:4], z_columns.at[j], w_s.at[2], w_r.at[2], z_peer[j]).start()
    for c in range(1, chunks):
        partner_copy(c).start()
    for j in range(1, GROUP):
        copy(bias, x_bias.at[j], w_s.at[3], w_r.at[3], u_peer[j]).start()

    def own_dense(layer):
        return dense(values[layer].astype(jnp.float32), own_columns[layer].astype(jnp.float32))

    w_end[0] = own_dense(0)

    def end_layer(own, other, which, layer):
        pair = jnp.concatenate([own, other], axis=1)
        preact = jnp.dot(pair, w_end[which], preferred_element_type=jnp.float32)
        return activate(preact + bias[layer : layer + 1, :])

    def first(c, _):
        partner_copy(c).wait_recv()
        for s in range(GROUP):
            act0[c, s] = end_layer(features[c, s], partner_in[c, s], 0, 0)
        for j in range(1, GROUP):
            copy(act0.at[c, z_of[j]], z_in.at[c, j], zi_s.at[c], zi_r.at[c], z_peer[j]).start()
        return 0

    lax.fori_loop(0, chunks, first, 0)

    def own_x(k, _):
        w_x[0, k] = own_dense(k + 4)
        return 0

    lax.fori_loop(0, 3, own_x, 0)
    for j in range(1, GROUP):
        copy(w_x.at[0], w_x.at[j], w_s.at[4], w_r.at[4], u_peer[j]).start()
    w_end[1] = own_dense(7)

    def many(ref, send, recv):
        return copy(ref.at[1:GROUP], ref.at[1:GROUP], send, recv, partner)

    for ref, at in ((z_bias, 0), (z_values, 1), (z_columns, 2)):
        many(ref, w_s.at[at], w_r.at[at]).wait_recv()

    def z_dense(i, _):
        j, k = i // 3, i % 3
        w_z[j, k] = dense(z_values[j, k].astype(jnp.float32), z_columns[j, k].astype(jnp.float32))
        return 0

    lax.fori_loop(0, 3 * GROUP, z_dense, 0)

    def z_layers(c, _):
        many(z_in.at[c], zi_s.at[c], zi_r.at[c]).wait_recv()
        slots = [act0[c, z]] + [z_in[c, j] for j in range(1, GROUP)]
        slots = three_layers(slots, w_z, z_bias, 1)
        back[c, 0] = slots[0]
        for j in range(1, GROUP):
            z_out[c, j] = slots[j]
        for j in range(1, GROUP):
            copy(z_out.at[c, j], back.at[c, j], zo_s.at[c], zo_r.at[c], z_peer[j]).start()
        return 0

    lax.fori_loop(0, chunks, z_layers, 0)
    many(x_bias, w_s.at[3], w_r.at[3]).wait_recv()
    many(w_x, w_s.at[4], w_r.at[4]).wait_recv()

    def to_x(c):
        many(back.at[c], zo_s.at[c], zo_r.at[c]).wait_recv()
        for j in range(1, GROUP):
            copy(back.at[c, u_of[j]], x_in.at[c, j], xi_s.at[c], xi_r.at[c], u_peer[j]).start()

    def x_layers(c):
        many(x_in.at[c], xi_s.at[c], xi_r.at[c]).wait_recv()
        slots = [back[c, u]] + [x_in[c, j] for j in range(1, GROUP)]
        slots = three_layers(slots, w_x, x_bias, 4)
        home[c, 0] = slots[0]
        for j in range(1, GROUP):
            x_out[c, j] = slots[j]
        for j in range(1, GROUP):
            copy(x_out.at[c, j], home.at[c, j], xo_s.at[c], xo_r.at[c], u_peer[j]).start()

    def last_copy(c):
        return copy(home.at[c], partner_home.at[c], pl_s.at[c], pl_r.at[c], partner)

    def to_partner(c):
        many(home.at[c], xo_s.at[c], xo_r.at[c]).wait_recv()
        last_copy(c).start()

    def last(c):
        last_copy(c).wait_recv()
        for j in range(GROUP):
            out[c, xor(zb, [(ub[k] + ((j >> k) & 1)) % 2 for k in range(3)])] = end_layer(
                home[c, j], partner_home[c, j], 1, LAYERS - 1
            )

    def steady(i, _):
        pl.when(i < chunks)(lambda: to_x(i))
        pl.when((i >= 1) & (i < chunks + 1))(lambda: x_layers(i - 1))
        pl.when((i >= 2) & (i < chunks + 2))(lambda: to_partner(i - 2))
        pl.when(i >= 3)(lambda: last(i - 3))
        return 0

    lax.fori_loop(0, chunks + 3, steady, 0)

    for ref, at in ((z_bias, 0), (z_values, 1), (z_columns, 2), (x_bias, 3), (w_x, 4)):
        many(ref, w_s.at[at], w_r.at[at]).wait_send()

    def drain(c, _):
        partner_copy(c).wait_send()
        last_copy(c).wait_send()
        many(z_in.at[c], zi_s.at[c], zi_r.at[c]).wait_send()
        many(z_out.at[c], zo_s.at[c], zo_r.at[c]).wait_send()
        many(x_in.at[c], xi_s.at[c], xi_r.at[c]).wait_send()
        many(x_out.at[c], xo_s.at[c], xo_r.at[c]).wait_send()
        return 0

    lax.fori_loop(0, chunks, drain, 0)


def shards(features, link_values, link_columns, layer_bias):
    rows, width = features.shape
    piece = rows // (CHUNKS * GROUP)
    tiled = (CHUNKS, GROUP, piece, width)
    layers, fan_in, _ = link_values.shape
    vmem = pl.BlockSpec(memory_space=pltpu.VMEM)
    act = pltpu.VMEM(tiled, jnp.bfloat16)
    links = pltpu.VMEM((GROUP, 3, fan_in, width), jnp.bfloat16)
    biases = pltpu.VMEM((GROUP, layers, width), jnp.float32)
    wide = pltpu.VMEM((GROUP, 3, 2 * width, width), jnp.bfloat16)
    out = pl.pallas_call(
        kernel,
        out_shape=jax.ShapeDtypeStruct(tiled, jnp.bfloat16),
        in_specs=[vmem] * 4,
        out_specs=vmem,
        scratch_shapes=[act] * 9
        + [
            pltpu.VMEM((layers, fan_in, width), jnp.bfloat16),
            links, links, biases, biases,
            pltpu.VMEM((2, 2 * width, width), jnp.bfloat16),
            wide, wide,
        ]
        + [pltpu.SemaphoreType.DMA((CHUNKS,))] * 12
        + [pltpu.SemaphoreType.DMA((5,))] * 2,
        compiler_params=pltpu.CompilerParams(
            collective_id=0, has_side_effects=True, vmem_limit_bytes=40 << 20
        ),
    )(features.reshape(tiled), link_values, link_columns, layer_bias)
    return out.reshape(rows, width)


def solution(mesh):
    return jax.shard_map(
        shards,
        mesh=mesh,
        in_specs=(P("row", "blk"), P(None, None, "blk"), P(None, None, "blk"), P(None, "blk")),
        out_specs=P("row", "blk"),
        check_vma=False,
    )
```

```python
import functools

import jax
import jax.numpy as jnp
from jax import lax
from jax.experimental import pallas as pl
from jax.experimental.pallas import tpu as pltpu
from jax.sharding import PartitionSpec as P

MESH = pl.DeviceIdType.MESH
LAYERS = 8
CEILING = 4.0
CHUNKS = 16
LAGS = (7, 10, 13, 14)
GROUP = 8
MASKS = (1, 2, 4)
FAR_FIRST = (4, 5, 7, 3, 6, 2, 1)
PARTS = 4
VMEM_LIMIT = 62 << 20


def bits(value):
    return [(value // 2**k) % 2 for k in range(3)]


def xor(value_bits, mask):
    total = 0
    for k in range(3):
        flip = (mask >> k) & 1 if isinstance(mask, int) else mask[k]
        total = total + ((value_bits[k] + flip) % 2) * 2**k
    return total


def dense(links):
    width = links[0][0].shape[1]
    field = lax.broadcasted_iota(jnp.int32, (2 * width, width), 0).astype(jnp.float32)
    total = jnp.zeros((2 * width, width), jnp.float32)
    for values, columns in links:
        for link in range(values.shape[0]):
            total = total + jnp.where(field == columns[link : link + 1, :], values[link : link + 1, :], 0.0)
    return total.astype(jnp.bfloat16)


def activate(preact):
    return jnp.minimum(jnp.maximum(preact, 0.0), CEILING).astype(jnp.bfloat16)


def three_layers(slots, weights, bias):
    width = slots[0].shape[1]
    for step, mask in enumerate(MASKS):
        after = [None] * GROUP
        for low in range(GROUP):
            if low & mask:
                continue
            high = low | mask
            w_low, w_high = weights[low, step], weights[high, step]
            w_high = jnp.concatenate([w_high[width:], w_high[:width]], axis=0)
            b_pair = jnp.concatenate([bias[low, step], bias[high, step]], axis=1)
            pair = jnp.dot(
                jnp.concatenate([slots[low], slots[high]], axis=1),
                jnp.concatenate([w_low, w_high], axis=1),
                preferred_element_type=jnp.float32,
            )
            pair = activate(pair + b_pair)
            after[low], after[high] = pair[:, :width], pair[:, width:]
        slots = after
    return slots


def kernel(
    features_hbm, values_hbm, columns_hbm, bias_hbm, out_hbm,
    features, values, columns, bias, out, partner_in, act0, z_in, z_out, back, x_in, x_out, home, partner_home,
    z_links, z_bias, x_bias, w_end, w_z, w_x,
    sent, pf_r, zi_r, zo_r, xi_r, xo_r, pl_r, w_r, local,
):
    chunks, _, piece, width = features.shape
    fan_in = values.shape[1]
    loads = [
        pltpu.make_async_copy(src, dst, local.at[k])
        for k, (src, dst) in enumerate(((values_hbm, values), (columns_hbm, columns), (bias_hbm, bias)))
    ]
    for one in loads:
        one.start()
    step = chunks // PARTS
    for k in range(PARTS):
        part = pl.ds(k * step, step)
        pltpu.make_async_copy(features_hbm.at[part], features.at[part], local.at[3]).start()

    block, row = lax.axis_index("blk"), lax.axis_index("row")
    core, z, u = block % 2, (block // 2) % GROUP, block // (2 * GROUP)
    zb, ub = bits(z), bits(u)
    z_of = [xor(zb, j) for j in range(GROUP)]
    u_of = [xor(ub, j) for j in range(GROUP)]
    z_peer = [{"blk": (u * GROUP + z_of[j]) * 2 + core} for j in range(GROUP)]
    u_peer = [{"blk": (u_of[j] * GROUP + z) * 2 + core} for j in range(GROUP)]
    partner, twin = {"blk": block + 1 - 2 * core}, {"row": 1 - row}

    def copy(src, dst, send, recv, peer):
        return pltpu.make_async_remote_copy(
            src_ref=src, dst_ref=dst, send_sem=sent.at[send], recv_sem=recv, device_id=peer, device_id_type=MESH
        )

    barrier = pltpu.get_barrier_semaphore()
    peers = [partner, twin, *z_peer[1:], *u_peer[1:]]
    for peer in peers:
        pl.semaphore_signal(barrier, inc=1, device_id=peer, device_id_type=MESH)
    for one in loads:
        one.wait()
    half = fan_in // 2
    for h in range(2):
        z_links[h, 0, 0] = values[1:4, h * half : (h + 1) * half, :]
        z_links[h, 0, 1] = columns[1:4, h * half : (h + 1) * half, :].astype(jnp.float32).astype(jnp.bfloat16)
    for k in range(3):
        z_bias[0, k] = bias[k + 1 : k + 2, :]
        x_bias[0, k] = bias[k + 4 : k + 5, :]
    pltpu.make_async_copy(features_hbm, features, local.at[3]).wait()
    with jax.named_scope("barrier"):
        pl.semaphore_wait(barrier, len(peers))

    def partner_copy(c):
        return copy(features.at[c], partner_in.at[c], 0, pf_r.at[c], partner)

    partner_copy(0).start()
    for j in FAR_FIRST:
        copy(z_links.at[row, 0], z_links.at[row, j], 6, w_r.at[0], z_peer[j]).start()
        copy(z_bias.at[0], z_bias.at[j], 7, w_r.at[1], z_peer[j]).start()
    for c in range(1, chunks):
        partner_copy(c).start()

    def own_dense(layer):
        return dense([(values[layer].astype(jnp.float32), columns[layer].astype(jnp.float32))])

    with jax.named_scope("w0"):
        w_end[0] = own_dense(0)

    def end_layer(own, other, which, layer):
        pair = jnp.concatenate([own, other], axis=1)
        preact = jnp.dot(pair, w_end[which], preferred_element_type=jnp.float32)
        return preact + bias[layer : layer + 1, :]

    def first(c, _):
        with jax.named_scope("pf_wait"):
            partner_copy(c).wait_recv()
        for s in range(GROUP):
            act0[c, s] = activate(end_layer(features[c, s], partner_in[c, s], 0, 0))
        for j in FAR_FIRST:
            copy(act0.at[c, z_of[j]], z_in.at[c, j], 1, zi_r.at[c], z_peer[j]).start()
        return 0

    lax.fori_loop(0, chunks, first, 0)

    def own_x(k, _):
        w_x[0, k] = own_dense(k + 4)
        return 0

    with jax.named_scope("own_x"):
        lax.fori_loop(0, 3, own_x, 0)
    w_end[1] = own_dense(7)

    def many(ref, send, recv):
        return copy(ref.at[1:GROUP], ref.at[1:GROUP], send, recv, partner)

    def links_from(r, peer, send, recv):
        return copy(z_links.at[r, 1:GROUP], z_links.at[r, 1:GROUP], send, recv, peer)

    with jax.named_scope("zw_wait"):
        links_from(row, twin, 6, w_r.at[0]).wait_recv()
    links_from(row, twin, 8, w_r.at[2]).start()
    for j in range(1, GROUP):
        copy(x_bias.at[0], x_bias.at[j], 9, w_r.at[3], u_peer[j]).start()
        copy(w_x.at[0], w_x.at[j], 10, w_r.at[4], u_peer[j]).start()
    with jax.named_scope("tw_wait"):
        many(z_bias, 7, w_r.at[1]).wait_recv()
        links_from(1 - row, twin, 8, w_r.at[2]).wait_recv()

    def z_dense(i, _):
        j, k = i // 3, i % 3
        w_z[j, k] = dense(
            [(z_links[h, j, 0, k].astype(jnp.float32), z_links[h, j, 1, k].astype(jnp.float32)) for h in range(2)]
        )
        return 0

    with jax.named_scope("z_dense"):
        lax.fori_loop(0, 3 * GROUP, z_dense, 0)

    def z_layers(c):
        with jax.named_scope("zin_wait"):
            many(z_in.at[c], 1, zi_r.at[c]).wait_recv()
        slots = [act0[c, z]] + [z_in[c, j] for j in range(1, GROUP)]
        slots = three_layers(slots, w_z, z_bias)
        back[c, 0] = slots[0]
        for j in range(1, GROUP):
            z_out[c, j] = slots[j]
        for j in FAR_FIRST:
            copy(z_out.at[c, j], back.at[c, j], 2, zo_r.at[c], z_peer[j]).start()

    def to_x(c):
        with jax.named_scope("zout_wait"):
            many(back.at[c], 2, zo_r.at[c]).wait_recv()
        for j in range(1, GROUP):
            copy(back.at[c, u_of[j]], x_in.at[c, j], 3, xi_r.at[c], u_peer[j]).start()

    def x_weights():
        with jax.named_scope("xw_wait"):
            many(x_bias, 9, w_r.at[3]).wait_recv()
            many(w_x, 10, w_r.at[4]).wait_recv()

    def x_layers(c):
        pl.when(c == 0)(x_weights)
        with jax.named_scope("xin_wait"):
            many(x_in.at[c], 3, xi_r.at[c]).wait_recv()
        slots = [back[c, u]] + [x_in[c, j] for j in range(1, GROUP)]
        slots = three_layers(slots, w_x, x_bias)
        home[c, 0] = slots[0]
        for j in range(1, GROUP):
            x_out[c, j] = slots[j]
        for j in range(1, GROUP):
            copy(x_out.at[c, j], home.at[c, j], 4, xo_r.at[c], u_peer[j]).start()

    def last_copy(c):
        return copy(home.at[c], partner_home.at[c], 5, pl_r.at[c], partner)

    def to_partner(c):
        with jax.named_scope("xout_wait"):
            many(home.at[c], 4, xo_r.at[c]).wait_recv()
        last_copy(c).start()

    def last(c):
        with jax.named_scope("pl_wait"):
            last_copy(c).wait_recv()
        for j in range(GROUP):
            preact = end_layer(home[c, j], partner_home[c, j], 1, LAYERS - 1)
            at = xor(zb, [(ub[k] + ((j >> k) & 1)) % 2 for k in range(3)])
            out[c, at] = jnp.minimum(preact, CEILING).astype(jnp.bfloat16)
        pltpu.make_async_copy(out.at[c], out_hbm.at[c], local.at[4]).start()

    def steady(i, _):
        pl.when(i < chunks)(lambda: z_layers(i))
        for stage, lag in zip((to_x, x_layers, to_partner, last), LAGS):
            pl.when((i >= lag) & (i < chunks + lag))(functools.partial(stage, i - lag))
        return 0

    lax.fori_loop(0, chunks + LAGS[-1], steady, 0)

    with jax.named_scope("drain"):
        for at, ref in (
            (0, features),
            (1, z_in.at[:, 1:GROUP]),
            (2, z_out.at[:, 1:GROUP]),
            (3, x_in.at[:, 1:GROUP]),
            (4, x_out.at[:, 1:GROUP]),
            (5, home),
            (6, z_links.at[0, 1:GROUP]),
            (7, z_bias.at[1:GROUP]),
            (8, z_links.at[0, 1:GROUP]),
            (9, x_bias.at[1:GROUP]),
            (10, w_x.at[1:GROUP]),
        ):
            copy(ref, ref, at, w_r.at[0], partner).wait_send()
        pltpu.make_async_copy(out, out_hbm, local.at[4]).wait()


def finish_kernel(source, result, before, after, arrived, stored):
    loads = [pltpu.make_async_copy(source.at[k], before.at[k], arrived.at[k]) for k in range(PARTS)]
    stores = [pltpu.make_async_copy(after.at[k], result.at[k], stored.at[k]) for k in range(PARTS)]
    for one in loads:
        one.start()
    for k in range(PARTS):
        loads[k].wait()
        after[k] = jnp.maximum(before[k], 0)
        stores[k].start()
    for one in stores:
        one.wait()


def shards(features, link_values, link_columns, layer_bias):
    rows, width = features.shape
    piece = rows // (CHUNKS * GROUP)
    tiled = (CHUNKS, GROUP, piece, width)
    layers, fan_in, _ = link_values.shape
    hbm = pl.BlockSpec(memory_space=pltpu.HBM)
    act = pltpu.VMEM(tiled, jnp.bfloat16)
    biases = pltpu.VMEM((GROUP, 3, 1, width), jnp.float32)
    wide = pltpu.VMEM((GROUP, 3, 2 * width, width), jnp.bfloat16)
    out = pl.pallas_call(
        kernel,
        out_shape=jax.ShapeDtypeStruct(tiled, jnp.bfloat16),
        in_specs=[hbm] * 4,
        out_specs=hbm,
        scratch_shapes=[
            act,
            pltpu.VMEM(link_values.shape, jnp.bfloat16),
            pltpu.VMEM(link_columns.shape, jnp.int32),
            pltpu.VMEM(layer_bias.shape, jnp.float32),
        ]
        + [act] * 10
        + [
            pltpu.VMEM((2, GROUP, 2, 3, fan_in // 2, width), jnp.bfloat16),
            biases,
            biases,
            pltpu.VMEM((2, 2 * width, width), jnp.bfloat16),
            wide,
            wide,
            pltpu.SemaphoreType.DMA((11,)),
        ]
        + [pltpu.SemaphoreType.DMA((CHUNKS,))] * 6
        + [pltpu.SemaphoreType.DMA((5,))] * 2,
        compiler_params=pltpu.CompilerParams(
            collective_id=0, has_side_effects=True, vmem_limit_bytes=VMEM_LIMIT
        ),
    )(features.reshape(tiled), link_values, link_columns, layer_bias)
    parts = (PARTS, rows // PARTS, width)
    result = pl.pallas_call(
        finish_kernel,
        out_shape=jax.ShapeDtypeStruct(parts, jnp.bfloat16),
        in_specs=[hbm],
        out_specs=hbm,
        scratch_shapes=[pltpu.VMEM(parts, jnp.bfloat16)] * 2 + [pltpu.SemaphoreType.DMA((PARTS,))] * 2,
        compiler_params=pltpu.CompilerParams(vmem_limit_bytes=VMEM_LIMIT),
    )(out.reshape(parts))
    return result.reshape(rows, width)


def solution(mesh):
    return jax.shard_map(
        shards,
        mesh=mesh,
        in_specs=(P("row", "blk"), P(None, None, "blk"), P(None, None, "blk"), P(None, "blk")),
        out_specs=P("row", "blk"),
        check_vma=False,
    )
```

```python
import functools

import jax
import jax.numpy as jnp
from jax import lax
from jax.experimental import pallas as pl
from jax.experimental.pallas import tpu as pltpu
from jax.sharding import PartitionSpec as P

MESH = pl.DeviceIdType.MESH
LAYERS = 8
CEILING = 4.0
CHUNKS = 16
LAGS = (7, 10, 13, 16)
GROUP = 8
MASKS = (1, 2, 4)
FAR_FIRST = (4, 5, 7, 3, 6, 2, 1)
X_FAR_FIRST = (5, 3, 7, 1, 4, 2, 6)
BOTH = 1
PARTS = 4
VMEM_LIMIT = 62 << 20


def bits(value):
    return [(value // 2**k) % 2 for k in range(3)]


def xor(value_bits, mask):
    total = 0
    for k in range(3):
        flip = (mask >> k) & 1 if isinstance(mask, int) else mask[k]
        total = total + ((value_bits[k] + flip) % 2) * 2**k
    return total


def dense(values, columns):
    width = values.shape[1]
    values, columns = values.astype(jnp.float32), columns.astype(jnp.float32)
    field = lax.broadcasted_iota(jnp.int32, (2 * width, width), 0).astype(jnp.float32)
    total = jnp.zeros((2 * width, width), jnp.float32)
    for link in range(values.shape[0]):
        total = total + jnp.where(field == columns[link : link + 1, :], values[link : link + 1, :], 0.0)
    return total


def activate(preact):
    return jnp.minimum(jnp.maximum(preact, 0.0), CEILING).astype(jnp.bfloat16)


def three_layers(slots, weights, bias):
    width = slots[0].shape[1]
    for step, mask in enumerate(MASKS):
        after = [None] * GROUP
        for low in range(GROUP):
            if low & mask:
                continue
            high = low | mask
            w_low, w_high = weights[low, step], weights[high, step]
            w_high = jnp.concatenate([w_high[width:], w_high[:width]], axis=0)
            b_pair = jnp.concatenate([bias[low, step], bias[high, step]], axis=1)
            pair = jnp.dot(
                jnp.concatenate([slots[low], slots[high]], axis=1),
                jnp.concatenate([w_low, w_high], axis=1),
                preferred_element_type=jnp.float32,
            )
            pair = activate(pair + b_pair)
            after[low], after[high] = pair[:, :width], pair[:, width:]
        slots = after
    return slots


def kernel(
    features_hbm, values_hbm, columns_hbm, bias_hbm, out_hbm,
    features, values, columns, bias, out, partner_in, act0, z_in, z_out, back, x_in, x_out, home, partner_home,
    partial, z_links, z_bias, x_bias, w_end, w_z, w_x,
    sent, pf_r, zi_r, zo_r, xi_r, xo_r, pl_r, w_r, local,
):
    chunks, _, piece, width = features.shape
    fan_in = values.shape[1]
    loads = [
        pltpu.make_async_copy(src, dst, local.at[k])
        for k, (src, dst) in enumerate(((values_hbm, values), (columns_hbm, columns), (bias_hbm, bias)))
    ]
    for one in loads:
        one.start()
    step = chunks // PARTS
    for k in range(PARTS):
        part = pl.ds(k * step, step)
        pltpu.make_async_copy(features_hbm.at[part], features.at[part], local.at[3]).start()

    block, row = lax.axis_index("blk"), lax.axis_index("row")
    core, z, u = block % 2, (block // 2) % GROUP, block // (2 * GROUP)
    zb, ub = bits(z), bits(u)
    z_of = [xor(zb, j) for j in range(GROUP)]
    u_of = [xor(ub, j) for j in range(GROUP)]
    z_peer = [{"blk": (u * GROUP + z_of[j]) * 2 + core} for j in range(GROUP)]
    u_peer = [{"blk": (u_of[j] * GROUP + z) * 2 + core} for j in range(GROUP)]
    other = [{"blk": (u_of[j] * GROUP + z) * 2 + 1 - core} for j in range(GROUP)]
    partner, twin = {"blk": block + 1 - 2 * core}, {"row": 1 - row}

    def copy(src, dst, send, recv, peer):
        return pltpu.make_async_remote_copy(
            src_ref=src, dst_ref=dst, send_sem=sent.at[send], recv_sem=recv, device_id=peer, device_id_type=MESH
        )

    barrier = pltpu.get_barrier_semaphore()
    peers = [partner, twin, *z_peer[1:], *u_peer[1:], *other[1:]]
    for peer in peers:
        pl.semaphore_signal(barrier, inc=1, device_id=peer, device_id_type=MESH)
    for one in loads:
        one.wait()
    half = fan_in // 2
    for h in range(2):
        z_links[h, 0, 0] = values[1:4, h * half : (h + 1) * half, :]
        z_links[h, 0, 1] = columns[1:4, h * half : (h + 1) * half, :].astype(jnp.float32).astype(jnp.bfloat16)
    for k in range(3):
        z_bias[0, k] = bias[k + 1 : k + 2, :]
        x_bias[0, k] = bias[k + 4 : k + 5, :]
    pltpu.make_async_copy(features_hbm, features, local.at[3]).wait()
    with jax.named_scope("barrier"):
        pl.semaphore_wait(barrier, len(peers))

    def partner_copy(c):
        return copy(features.at[c], partner_in.at[c], 0, pf_r.at[c], partner)

    partner_copy(0).start()
    for j in FAR_FIRST:
        copy(z_links.at[row, 0], z_links.at[row, j], 6, w_r.at[0], z_peer[j]).start()
        copy(z_bias.at[0], z_bias.at[j], 7, w_r.at[1], z_peer[j]).start()
    for c in range(1, chunks):
        partner_copy(c).start()

    def own_dense(layer):
        return dense(values[layer], columns[layer]).astype(jnp.bfloat16)

    with jax.named_scope("w0"):
        w_end[0] = own_dense(0)

    def end_layer(own, other, which, layer):
        pair = jnp.concatenate([own, other], axis=1)
        preact = jnp.dot(pair, w_end[which], preferred_element_type=jnp.float32)
        return preact + bias[layer : layer + 1, :]

    def first(c, _):
        with jax.named_scope("pf_wait"):
            partner_copy(c).wait_recv()
        for s in range(GROUP):
            act0[c, s] = activate(end_layer(features[c, s], partner_in[c, s], 0, 0))
        for j in FAR_FIRST:
            copy(act0.at[c, z_of[j]], z_in.at[c, j], 1, zi_r.at[c], z_peer[j]).start()
        return 0

    lax.fori_loop(0, chunks, first, 0)

    def own_x(k, _):
        w_x[0, k] = own_dense(k + 4)
        return 0

    with jax.named_scope("own_x"):
        lax.fori_loop(0, 3, own_x, 0)
    w_end[1] = own_dense(7)

    def many(ref, send, recv):
        return copy(ref.at[1:GROUP], ref.at[1:GROUP], send, recv, partner)

    def links_from(r, peer, send, recv):
        return copy(z_links.at[r, 1:GROUP], z_links.at[r, 1:GROUP], send, recv, peer)

    def loop(first_step, last_step, body):
        lax.fori_loop(first_step, last_step, lambda i, _: (body(i), 0)[1], 0)

    def send_w_x(j):
        copy(x_bias.at[0], x_bias.at[j], 9, w_r.at[3], u_peer[j]).start()
        copy(w_x.at[0], w_x.at[j], 10, w_r.at[4], u_peer[j]).start()

    for j in (2, 4, 6):
        send_w_x(j)

    def z_own(k):
        w_z[0, k] = own_dense(k + 1)

    def z_half(h, i):
        return dense(z_links[h, i // 3, 0, i % 3], z_links[h, i // 3, 1, i % 3])

    def z_first(i):
        partial[i // 3, i % 3] = z_half(row, i)

    def z_second(i):
        w_z[i // 3, i % 3] = (partial[i // 3, i % 3] + z_half(1 - row, i)).astype(jnp.bfloat16)

    loop(0, 3, z_own)
    with jax.named_scope("zw_wait"):
        links_from(row, twin, 6, w_r.at[0]).wait_recv()
    links_from(row, twin, 8, w_r.at[2]).start()
    for j in (1, 5, 3, 7):
        send_w_x(j)
    with jax.named_scope("z_first"):
        loop(3, 3 * GROUP, z_first)
    with jax.named_scope("tw_wait"):
        many(z_bias, 7, w_r.at[1]).wait_recv()
        links_from(1 - row, twin, 8, w_r.at[2]).wait_recv()
    with jax.named_scope("z_dense"):
        loop(3, 3 * GROUP, z_second)

    def z_layers(c):
        with jax.named_scope("zin_wait"):
            many(z_in.at[c], 1, zi_r.at[c]).wait_recv()
        slots = [act0[c, z]] + [z_in[c, j] for j in range(1, GROUP)]
        slots = three_layers(slots, w_z, z_bias)
        back[c, 0] = slots[0]
        for j in range(1, GROUP):
            z_out[c, j] = slots[j]
        for j in FAR_FIRST:
            copy(z_out.at[c, j], back.at[c, j], 2, zo_r.at[c], z_peer[j]).start()

    def to_x(c):
        with jax.named_scope("zout_wait"):
            many(back.at[c], 2, zo_r.at[c]).wait_recv()
        for j in X_FAR_FIRST:
            copy(back.at[c, u_of[j]], x_in.at[c, j], 3, xi_r.at[c], u_peer[j]).start()

    def x_weights():
        with jax.named_scope("xw_wait"):
            many(x_bias, 9, w_r.at[3]).wait_recv()
            many(w_x, 10, w_r.at[4]).wait_recv()

    def x_layers(c):
        pl.when(c == 0)(x_weights)
        with jax.named_scope("xin_wait"):
            many(x_in.at[c], 3, xi_r.at[c]).wait_recv()
        slots = [back[c, u]] + [x_in[c, j] for j in range(1, GROUP)]
        slots = three_layers(slots, w_x, x_bias)
        home[c, 0] = slots[0]
        for j in range(1, GROUP):
            x_out[c, j] = slots[j]

        def to_both():
            for j in X_FAR_FIRST:
                copy(x_out.at[c, j], home.at[c, j], 4, xo_r.at[c], u_peer[j]).start()
                copy(x_out.at[c, j], partner_home.at[c, j], 5, pl_r.at[c], other[j]).start()
            copy(home.at[c, 0], partner_home.at[c, 0], 5, pl_r.at[c], partner).start()

        def to_one():
            for j in X_FAR_FIRST:
                copy(x_out.at[c, j], home.at[c, j], 4, xo_r.at[c], u_peer[j]).start()

        pl.when(c >= chunks - BOTH)(to_both)
        pl.when(c < chunks - BOTH)(to_one)

    def last_copy(c):
        return copy(home.at[c], partner_home.at[c], 5, pl_r.at[c], partner)

    def to_partner(c):
        with jax.named_scope("xout_wait"):
            many(home.at[c], 4, xo_r.at[c]).wait_recv()
        pl.when(c < chunks - BOTH)(lambda: last_copy(c).start())

    def last(c):
        with jax.named_scope("pl_wait"):
            last_copy(c).wait_recv()
        for j in range(GROUP):
            preact = end_layer(home[c, j], partner_home[c, j], 1, LAYERS - 1)
            at = xor(zb, [(ub[k] + ((j >> k) & 1)) % 2 for k in range(3)])
            out[c, at] = jnp.minimum(preact, CEILING).astype(jnp.bfloat16)
        pltpu.make_async_copy(out.at[c], out_hbm.at[c], local.at[4]).start()

    def steady(i, _):
        pl.when(i < chunks)(lambda: z_layers(i))
        for stage, lag in zip((to_x, x_layers, to_partner, last), LAGS):
            pl.when((i >= lag) & (i < chunks + lag))(functools.partial(stage, i - lag))
        return 0

    lax.fori_loop(0, chunks + LAGS[-1], steady, 0)

    with jax.named_scope("drain"):
        for at, ref in (
            (0, features),
            (1, z_in.at[:, 1:GROUP]),
            (2, z_out.at[:, 1:GROUP]),
            (3, x_in.at[:, 1:GROUP]),
            (4, x_out.at[:, 1:GROUP]),
            (5, home),
            (6, z_links.at[0, 1:GROUP]),
            (7, z_bias.at[1:GROUP]),
            (8, z_links.at[0, 1:GROUP]),
            (9, x_bias.at[1:GROUP]),
            (10, w_x.at[1:GROUP]),
        ):
            copy(ref, ref, at, w_r.at[0], partner).wait_send()
        pltpu.make_async_copy(out, out_hbm, local.at[4]).wait()


def finish_kernel(source, result, before, after, arrived, stored):
    loads = [pltpu.make_async_copy(source.at[k], before.at[k], arrived.at[k]) for k in range(PARTS)]
    stores = [pltpu.make_async_copy(after.at[k], result.at[k], stored.at[k]) for k in range(PARTS)]
    for one in loads:
        one.start()
    for k in range(PARTS):
        loads[k].wait()
        after[k] = jnp.maximum(before[k], 0)
        stores[k].start()
    for one in stores:
        one.wait()


def shards(features, link_values, link_columns, layer_bias):
    rows, width = features.shape
    piece = rows // (CHUNKS * GROUP)
    tiled = (CHUNKS, GROUP, piece, width)
    layers, fan_in, _ = link_values.shape
    hbm = pl.BlockSpec(memory_space=pltpu.HBM)
    act = pltpu.VMEM(tiled, jnp.bfloat16)
    biases = pltpu.VMEM((GROUP, 3, 1, width), jnp.float32)
    wide = pltpu.VMEM((GROUP, 3, 2 * width, width), jnp.bfloat16)
    out = pl.pallas_call(
        kernel,
        out_shape=jax.ShapeDtypeStruct(tiled, jnp.bfloat16),
        in_specs=[hbm] * 4,
        out_specs=hbm,
        scratch_shapes=[
            act,
            pltpu.VMEM(link_values.shape, jnp.bfloat16),
            pltpu.VMEM(link_columns.shape, jnp.int32),
            pltpu.VMEM(layer_bias.shape, jnp.float32),
        ]
        + [act] * 10
        + [
            pltpu.VMEM((GROUP, 3, 2 * width, width), jnp.float32),
            pltpu.VMEM((2, GROUP, 2, 3, fan_in // 2, width), jnp.bfloat16),
            biases,
            biases,
            pltpu.VMEM((2, 2 * width, width), jnp.bfloat16),
            wide,
            wide,
            pltpu.SemaphoreType.DMA((11,)),
        ]
        + [pltpu.SemaphoreType.DMA((CHUNKS,))] * 6
        + [pltpu.SemaphoreType.DMA((5,))] * 2,
        compiler_params=pltpu.CompilerParams(
            collective_id=0, has_side_effects=True, vmem_limit_bytes=VMEM_LIMIT
        ),
    )(features.reshape(tiled), link_values, link_columns, layer_bias)
    parts = (PARTS, rows // PARTS, width)
    result = pl.pallas_call(
        finish_kernel,
        out_shape=jax.ShapeDtypeStruct(parts, jnp.bfloat16),
        in_specs=[hbm],
        out_specs=hbm,
        scratch_shapes=[pltpu.VMEM(parts, jnp.bfloat16)] * 2 + [pltpu.SemaphoreType.DMA((PARTS,))] * 2,
        compiler_params=pltpu.CompilerParams(vmem_limit_bytes=VMEM_LIMIT),
    )(out.reshape(parts))
    return result.reshape(rows, width)


def solution(mesh):
    return jax.shard_map(
        shards,
        mesh=mesh,
        in_specs=(P("row", "blk"), P(None, None, "blk"), P(None, None, "blk"), P(None, "blk")),
        out_specs=P("row", "blk"),
        check_vma=False,
    )
```

```python
import functools

import jax
import jax.numpy as jnp
from jax import lax
from jax.experimental import pallas as pl
from jax.experimental.pallas import tpu as pltpu
from jax.sharding import PartitionSpec as P

MESH = pl.DeviceIdType.MESH
LAYERS = 8
CEILING = 4.0
CHUNKS = 12
LAGS = (5, 7, 9, 11)
GROUP = 8
MASKS = (1, 2, 4)
FAR_FIRST = (4, 5, 7, 3, 6, 2, 1)
X_FAR_FIRST = (5, 7, 3, 4, 1, 6, 2)
BOTH = 1
PARTS = 4
VMEM_LIMIT = 62 << 20


def bits(value):
    return [(value // 2**k) % 2 for k in range(3)]


def xor(value_bits, mask):
    total = 0
    for k in range(3):
        flip = (mask >> k) & 1 if isinstance(mask, int) else mask[k]
        total = total + ((value_bits[k] + flip) % 2) * 2**k
    return total


def dense(values, columns):
    width = values.shape[1]
    values, columns = values.astype(jnp.float32), columns.astype(jnp.float32)
    field = lax.broadcasted_iota(jnp.int32, (2 * width, width), 0).astype(jnp.float32)
    total = jnp.zeros((2 * width, width), jnp.float32)
    for link in range(values.shape[0]):
        total = total + jnp.where(field == columns[link : link + 1, :], values[link : link + 1, :], 0.0)
    return total


def activate(preact):
    return jnp.minimum(jnp.maximum(preact, 0.0), CEILING).astype(jnp.bfloat16)


def three_layers(slots, weights, bias):
    width = slots[0].shape[1]
    for step, mask in enumerate(MASKS):
        after = [None] * GROUP
        for low in range(GROUP):
            if low & mask:
                continue
            high = low | mask
            w_low, w_high = weights[low, step], weights[high, step]
            w_high = jnp.concatenate([w_high[width:], w_high[:width]], axis=0)
            b_pair = jnp.concatenate([bias[low, step], bias[high, step]], axis=1)
            pair = jnp.dot(
                jnp.concatenate([slots[low], slots[high]], axis=1),
                jnp.concatenate([w_low, w_high], axis=1),
                preferred_element_type=jnp.float32,
            )
            pair = activate(pair + b_pair)
            after[low], after[high] = pair[:, :width], pair[:, width:]
        slots = after
    return slots


def kernel(
    features_hbm, values_hbm, columns_hbm, bias_hbm, out_hbm,
    features, values, columns, bias, out, partner_in, act0, z_in, z_out, back, x_in, x_out, home, partner_home,
    partial, z_links, z_bias, x_bias, w_end, w_z, w_x,
    sent, pf_r, zi_r, zo_r, xi_r, xo_r, pl_r, w_r, local,
):
    chunks, _, piece, width = features.shape
    fan_in = values.shape[1]
    loads = [
        pltpu.make_async_copy(src, dst, local.at[k])
        for k, (src, dst) in enumerate(((values_hbm, values), (columns_hbm, columns), (bias_hbm, bias)))
    ]
    for one in loads:
        one.start()
    step = chunks // PARTS
    for k in range(PARTS):
        part = pl.ds(k * step, step)
        pltpu.make_async_copy(features_hbm.at[part], features.at[part], local.at[3]).start()

    block, row = lax.axis_index("blk"), lax.axis_index("row")
    core, z, u = block % 2, (block // 2) % GROUP, block // (2 * GROUP)
    zb, ub = bits(z), bits(u)
    z_of = [xor(zb, j) for j in range(GROUP)]
    u_of = [xor(ub, j) for j in range(GROUP)]
    z_peer = [{"blk": (u * GROUP + z_of[j]) * 2 + core} for j in range(GROUP)]
    u_peer = [{"blk": (u_of[j] * GROUP + z) * 2 + core} for j in range(GROUP)]
    other = [{"blk": (u_of[j] * GROUP + z) * 2 + 1 - core} for j in range(GROUP)]
    partner, twin = {"blk": block + 1 - 2 * core}, {"row": 1 - row}

    def copy(src, dst, send, recv, peer):
        return pltpu.make_async_remote_copy(
            src_ref=src, dst_ref=dst, send_sem=sent.at[send], recv_sem=recv, device_id=peer, device_id_type=MESH
        )

    barrier = pltpu.get_barrier_semaphore()
    peers = [partner, twin, *z_peer[1:], *u_peer[1:], *other[1:]]
    for peer in peers:
        pl.semaphore_signal(barrier, inc=1, device_id=peer, device_id_type=MESH)
    for one in loads:
        one.wait()
    half = fan_in // 2
    for h in range(2):
        z_links[h, 0, 0] = values[1:4, h * half : (h + 1) * half, :]
        z_links[h, 0, 1] = columns[1:4, h * half : (h + 1) * half, :].astype(jnp.float32).astype(jnp.bfloat16)
    for k in range(3):
        z_bias[0, k] = bias[k + 1 : k + 2, :]
        x_bias[0, k] = bias[k + 4 : k + 5, :]
    pltpu.make_async_copy(features_hbm, features, local.at[3]).wait()
    with jax.named_scope("barrier"):
        pl.semaphore_wait(barrier, len(peers))

    def partner_copy(c):
        return copy(features.at[c], partner_in.at[c], 0, pf_r.at[c], partner)

    partner_copy(0).start()
    for j in FAR_FIRST:
        copy(z_links.at[row, 0], z_links.at[row, j], 6, w_r.at[0], z_peer[j]).start()
        copy(z_bias.at[0], z_bias.at[j], 7, w_r.at[1], z_peer[j]).start()
    for c in range(1, chunks):
        partner_copy(c).start()

    def own_dense(layer):
        return dense(values[layer], columns[layer]).astype(jnp.bfloat16)

    with jax.named_scope("w0"):
        w_end[0] = own_dense(0)

    def end_layer(own, other, which, layer):
        pair = jnp.concatenate([own, other], axis=1)
        preact = jnp.dot(pair, w_end[which], preferred_element_type=jnp.float32)
        return preact + bias[layer : layer + 1, :]

    def first(c, _):
        with jax.named_scope("pf_wait"):
            partner_copy(c).wait_recv()
        for s in range(GROUP):
            act0[c, s] = activate(end_layer(features[c, s], partner_in[c, s], 0, 0))
        for j in FAR_FIRST:
            copy(act0.at[c, z_of[j]], z_in.at[c, j], 1, zi_r.at[c], z_peer[j]).start()
        return 0

    lax.fori_loop(0, chunks, first, 0)

    def own_x(k, _):
        w_x[0, k] = own_dense(k + 4)
        return 0

    with jax.named_scope("own_x"):
        lax.fori_loop(0, 3, own_x, 0)
    w_end[1] = own_dense(7)

    def many(ref, send, recv):
        return copy(ref.at[1:GROUP], ref.at[1:GROUP], send, recv, partner)

    def links_from(r, peer, send, recv):
        return copy(z_links.at[r, 1:GROUP], z_links.at[r, 1:GROUP], send, recv, peer)

    def loop(first_step, last_step, body):
        lax.fori_loop(first_step, last_step, lambda i, _: (body(i), 0)[1], 0)

    def send_w_x(j):
        copy(x_bias.at[0], x_bias.at[j], 9, w_r.at[3], u_peer[j]).start()
        copy(w_x.at[0], w_x.at[j], 10, w_r.at[4], u_peer[j]).start()

    for j in (2, 4, 6):
        send_w_x(j)

    def z_own(k):
        w_z[0, k] = own_dense(k + 1)

    def z_half(h, i):
        return dense(z_links[h, i // 3, 0, i % 3], z_links[h, i // 3, 1, i % 3])

    def z_first(i):
        partial[i // 3, i % 3] = z_half(row, i)

    def z_second(i):
        w_z[i // 3, i % 3] = (partial[i // 3, i % 3] + z_half(1 - row, i)).astype(jnp.bfloat16)

    loop(0, 3, z_own)
    with jax.named_scope("zw_wait"):
        links_from(row, twin, 6, w_r.at[0]).wait_recv()
    links_from(row, twin, 8, w_r.at[2]).start()
    for j in (1, 5, 3, 7):
        send_w_x(j)
    with jax.named_scope("z_first"):
        loop(3, 3 * GROUP, z_first)
    with jax.named_scope("tw_wait"):
        many(z_bias, 7, w_r.at[1]).wait_recv()
        links_from(1 - row, twin, 8, w_r.at[2]).wait_recv()
    with jax.named_scope("z_dense"):
        loop(3, 3 * GROUP, z_second)

    def z_layers(c):
        with jax.named_scope("zin_wait"):
            many(z_in.at[c], 1, zi_r.at[c]).wait_recv()
        slots = [act0[c, z]] + [z_in[c, j] for j in range(1, GROUP)]
        slots = three_layers(slots, w_z, z_bias)
        back[c, 0] = slots[0]
        for j in range(1, GROUP):
            z_out[c, j] = slots[j]
        for j in FAR_FIRST:
            copy(z_out.at[c, j], back.at[c, j], 2, zo_r.at[c], z_peer[j]).start()

    def to_x(c):
        with jax.named_scope("zout_wait"):
            many(back.at[c], 2, zo_r.at[c]).wait_recv()
        for j in X_FAR_FIRST:
            copy(back.at[c, u_of[j]], x_in.at[c, j], 3, xi_r.at[c], u_peer[j]).start()

    def x_weights():
        with jax.named_scope("xw_wait"):
            many(x_bias, 9, w_r.at[3]).wait_recv()
            many(w_x, 10, w_r.at[4]).wait_recv()

    def x_layers(c):
        pl.when(c == 0)(x_weights)
        with jax.named_scope("xin_wait"):
            many(x_in.at[c], 3, xi_r.at[c]).wait_recv()
        slots = [back[c, u]] + [x_in[c, j] for j in range(1, GROUP)]
        slots = three_layers(slots, w_x, x_bias)
        home[c, 0] = slots[0]
        for j in range(1, GROUP):
            x_out[c, j] = slots[j]

        def to_both():
            for j in X_FAR_FIRST:
                copy(x_out.at[c, j], home.at[c, j], 4, xo_r.at[c], u_peer[j]).start()
                copy(x_out.at[c, j], partner_home.at[c, j], 5, pl_r.at[c], other[j]).start()
            copy(home.at[c, 0], partner_home.at[c, 0], 5, pl_r.at[c], partner).start()

        def to_one():
            for j in X_FAR_FIRST:
                copy(x_out.at[c, j], home.at[c, j], 4, xo_r.at[c], u_peer[j]).start()

        pl.when(c >= chunks - BOTH)(to_both)
        pl.when(c < chunks - BOTH)(to_one)

    def last_copy(c):
        return copy(home.at[c], partner_home.at[c], 5, pl_r.at[c], partner)

    def to_partner(c):
        with jax.named_scope("xout_wait"):
            many(home.at[c], 4, xo_r.at[c]).wait_recv()
        pl.when(c < chunks - BOTH)(lambda: last_copy(c).start())

    def last(c):
        with jax.named_scope("pl_wait"):
            last_copy(c).wait_recv()
        for j in range(GROUP):
            preact = end_layer(home[c, j], partner_home[c, j], 1, LAYERS - 1)
            at = xor(zb, [(ub[k] + ((j >> k) & 1)) % 2 for k in range(3)])
            out[c, at] = jnp.minimum(preact, CEILING).astype(jnp.bfloat16)
        pltpu.make_async_copy(out.at[c], out_hbm.at[c], local.at[4]).start()

    def steady(i, _):
        pl.when(i < chunks)(lambda: z_layers(i))
        for stage, lag in zip((to_x, x_layers, to_partner, last), LAGS):
            pl.when((i >= lag) & (i < chunks + lag))(functools.partial(stage, i - lag))
        return 0

    lax.fori_loop(0, chunks + LAGS[-1], steady, 0)

    with jax.named_scope("drain"):
        for at, ref in (
            (0, features),
            (1, z_in.at[:, 1:GROUP]),
            (2, z_out.at[:, 1:GROUP]),
            (3, x_in.at[:, 1:GROUP]),
            (4, x_out.at[:, 1:GROUP]),
            (5, home),
            (6, z_links.at[0, 1:GROUP]),
            (7, z_bias.at[1:GROUP]),
            (8, z_links.at[0, 1:GROUP]),
            (9, x_bias.at[1:GROUP]),
            (10, w_x.at[1:GROUP]),
        ):
            copy(ref, ref, at, w_r.at[0], partner).wait_send()
        pltpu.make_async_copy(out, out_hbm, local.at[4]).wait()


def finish_kernel(source, result, before, after, arrived, stored):
    loads = [pltpu.make_async_copy(source.at[k], before.at[k], arrived.at[k]) for k in range(PARTS)]
    stores = [pltpu.make_async_copy(after.at[k], result.at[k], stored.at[k]) for k in range(PARTS)]
    for one in loads:
        one.start()
    for k in range(PARTS):
        loads[k].wait()
        after[k] = jnp.maximum(before[k], 0)
        stores[k].start()
    for one in stores:
        one.wait()


def shards(features, link_values, link_columns, layer_bias):
    rows, width = features.shape
    piece = rows // (CHUNKS * GROUP)
    tiled = (CHUNKS, GROUP, piece, width)
    layers, fan_in, _ = link_values.shape
    hbm = pl.BlockSpec(memory_space=pltpu.HBM)
    act = pltpu.VMEM(tiled, jnp.bfloat16)
    biases = pltpu.VMEM((GROUP, 3, 1, width), jnp.float32)
    wide = pltpu.VMEM((GROUP, 3, 2 * width, width), jnp.bfloat16)
    out = pl.pallas_call(
        kernel,
        out_shape=jax.ShapeDtypeStruct(tiled, jnp.bfloat16),
        in_specs=[hbm] * 4,
        out_specs=hbm,
        scratch_shapes=[
            act,
            pltpu.VMEM(link_values.shape, jnp.bfloat16),
            pltpu.VMEM(link_columns.shape, jnp.int32),
            pltpu.VMEM(layer_bias.shape, jnp.float32),
        ]
        + [act] * 10
        + [
            pltpu.VMEM((GROUP, 3, 2 * width, width), jnp.float32),
            pltpu.VMEM((2, GROUP, 2, 3, fan_in // 2, width), jnp.bfloat16),
            biases,
            biases,
            pltpu.VMEM((2, 2 * width, width), jnp.bfloat16),
            wide,
            wide,
            pltpu.SemaphoreType.DMA((11,)),
        ]
        + [pltpu.SemaphoreType.DMA((CHUNKS,))] * 6
        + [pltpu.SemaphoreType.DMA((5,))] * 2,
        compiler_params=pltpu.CompilerParams(
            collective_id=0, has_side_effects=True, vmem_limit_bytes=VMEM_LIMIT
        ),
    )(features.reshape(tiled), link_values, link_columns, layer_bias)
    parts = (PARTS, rows // PARTS, width)
    result = pl.pallas_call(
        finish_kernel,
        out_shape=jax.ShapeDtypeStruct(parts, jnp.bfloat16),
        in_specs=[hbm],
        out_specs=hbm,
        scratch_shapes=[pltpu.VMEM(parts, jnp.bfloat16)] * 2 + [pltpu.SemaphoreType.DMA((PARTS,))] * 2,
        compiler_params=pltpu.CompilerParams(vmem_limit_bytes=VMEM_LIMIT),
    )(out.reshape(parts))
    return result.reshape(rows, width)


def solution(mesh):
    return jax.shard_map(
        shards,
        mesh=mesh,
        in_specs=(P("row", "blk"), P(None, None, "blk"), P(None, None, "blk"), P(None, "blk")),
        out_specs=P("row", "blk"),
        check_vma=False,
    )
```

```python
import functools

import jax
import jax.numpy as jnp
from jax import lax
from jax.experimental import pallas as pl
from jax.experimental.pallas import tpu as pltpu
from jax.sharding import PartitionSpec as P

MESH = pl.DeviceIdType.MESH
LAYERS = 8
CEILING = 4.0
CHUNKS = 12
LAGS = (5, 7, 9, 11)
GROUP = 8
MASKS = (1, 2, 4)
FAR_FIRST = (4, 5, 7, 3, 6, 2, 1)
X_FAR_FIRST = (5, 7, 3, 4, 1, 6, 2)
BOTH = 2
PARTS = 4
VMEM_LIMIT = 62 << 20


def bits(value):
    return [(value // 2**k) % 2 for k in range(3)]


def xor(value_bits, mask):
    total = 0
    for k in range(3):
        flip = (mask >> k) & 1 if isinstance(mask, int) else mask[k]
        total = total + ((value_bits[k] + flip) % 2) * 2**k
    return total


def dense(values, columns):
    width = values.shape[1]
    values, columns = values.astype(jnp.float32), columns.astype(jnp.float32)
    field = lax.broadcasted_iota(jnp.int32, (2 * width, width), 0).astype(jnp.float32)
    total = jnp.zeros((2 * width, width), jnp.float32)
    for link in range(values.shape[0]):
        total = total + jnp.where(field == columns[link : link + 1, :], values[link : link + 1, :], 0.0)
    return total


def activate(preact):
    return jnp.minimum(jnp.maximum(preact, 0.0), CEILING).astype(jnp.bfloat16)


def three_layers(slots, weights, bias):
    width = slots[0].shape[1]
    for step, mask in enumerate(MASKS):
        after = [None] * GROUP
        for low in range(GROUP):
            if low & mask:
                continue
            high = low | mask
            w_low, w_high = weights[low, step], weights[high, step]
            w_high = jnp.concatenate([w_high[width:], w_high[:width]], axis=0)
            b_pair = jnp.concatenate([bias[low, step], bias[high, step]], axis=1)
            pair = jnp.dot(
                jnp.concatenate([slots[low], slots[high]], axis=1),
                jnp.concatenate([w_low, w_high], axis=1),
                preferred_element_type=jnp.float32,
            )
            pair = activate(pair + b_pair)
            after[low], after[high] = pair[:, :width], pair[:, width:]
        slots = after
    return slots


def kernel(
    features_hbm, values_hbm, columns_hbm, bias_hbm, out_hbm,
    features, values, columns, bias, out, partner_in, act0, z_in, z_out, back, x_in, x_out, home, partner_home,
    partial, z_links, z_bias, x_bias, w_end, w_z, w_x,
    sent, pf_r, zi_r, zo_r, xi_r, xo_r, pl_r, w_r, local,
):
    chunks, _, piece, width = features.shape
    fan_in = values.shape[1]
    loads = [
        pltpu.make_async_copy(src, dst, local.at[k])
        for k, (src, dst) in enumerate(((values_hbm, values), (columns_hbm, columns), (bias_hbm, bias)))
    ]
    for one in loads:
        one.start()
    step = chunks // PARTS
    for k in range(PARTS):
        part = pl.ds(k * step, step)
        pltpu.make_async_copy(features_hbm.at[part], features.at[part], local.at[3]).start()

    block, row = lax.axis_index("blk"), lax.axis_index("row")
    core, z, u = block % 2, (block // 2) % GROUP, block // (2 * GROUP)
    zb, ub = bits(z), bits(u)
    z_of = [xor(zb, j) for j in range(GROUP)]
    u_of = [xor(ub, j) for j in range(GROUP)]
    z_peer = [{"blk": (u * GROUP + z_of[j]) * 2 + core} for j in range(GROUP)]
    u_peer = [{"blk": (u_of[j] * GROUP + z) * 2 + core} for j in range(GROUP)]
    other = [{"blk": (u_of[j] * GROUP + z) * 2 + 1 - core} for j in range(GROUP)]
    partner, twin = {"blk": block + 1 - 2 * core}, {"row": 1 - row}

    def copy(src, dst, send, recv, peer):
        return pltpu.make_async_remote_copy(
            src_ref=src, dst_ref=dst, send_sem=sent.at[send], recv_sem=recv, device_id=peer, device_id_type=MESH
        )

    barrier = pltpu.get_barrier_semaphore()
    peers = [partner, twin, *z_peer[1:], *u_peer[1:], *other[1:]]
    for peer in peers:
        pl.semaphore_signal(barrier, inc=1, device_id=peer, device_id_type=MESH)
    for one in loads:
        one.wait()
    half = fan_in // 2
    for h in range(2):
        z_links[h, 0, 0] = values[1:4, h * half : (h + 1) * half, :]
        z_links[h, 0, 1] = columns[1:4, h * half : (h + 1) * half, :].astype(jnp.float32).astype(jnp.bfloat16)
    for k in range(3):
        z_bias[0, k] = bias[k + 1 : k + 2, :]
        x_bias[0, k] = bias[k + 4 : k + 5, :]
    pltpu.make_async_copy(features_hbm, features, local.at[3]).wait()
    with jax.named_scope("barrier"):
        pl.semaphore_wait(barrier, len(peers))

    def partner_copy(c):
        return copy(features.at[c], partner_in.at[c], 0, pf_r.at[c], partner)

    partner_copy(0).start()
    for j in FAR_FIRST:
        copy(z_links.at[row, 0], z_links.at[row, j], 6, w_r.at[0], z_peer[j]).start()
        copy(z_bias.at[0], z_bias.at[j], 7, w_r.at[1], z_peer[j]).start()
    for c in range(1, chunks):
        partner_copy(c).start()

    def own_dense(layer):
        return dense(values[layer], columns[layer]).astype(jnp.bfloat16)

    with jax.named_scope("w0"):
        w_end[0] = own_dense(0)

    def end_layer(own, other, which, layer):
        pair = jnp.concatenate([own, other], axis=1)
        preact = jnp.dot(pair, w_end[which], preferred_element_type=jnp.float32)
        return preact + bias[layer : layer + 1, :]

    def first(c, _):
        with jax.named_scope("pf_wait"):
            partner_copy(c).wait_recv()
        for s in range(GROUP):
            act0[c, s] = activate(end_layer(features[c, s], partner_in[c, s], 0, 0))
        for j in FAR_FIRST:
            copy(act0.at[c, z_of[j]], z_in.at[c, j], 1, zi_r.at[c], z_peer[j]).start()
        return 0

    lax.fori_loop(0, chunks, first, 0)

    def own_x(k, _):
        w_x[0, k] = own_dense(k + 4)
        return 0

    with jax.named_scope("own_x"):
        lax.fori_loop(0, 3, own_x, 0)
    w_end[1] = own_dense(7)

    def many(ref, send, recv):
        return copy(ref.at[1:GROUP], ref.at[1:GROUP], send, recv, partner)

    def links_from(r, peer, send, recv):
        return copy(z_links.at[r, 1:GROUP], z_links.at[r, 1:GROUP], send, recv, peer)

    def loop(first_step, last_step, body):
        lax.fori_loop(first_step, last_step, lambda i, _: (body(i), 0)[1], 0)

    def send_w_x(j):
        copy(x_bias.at[0], x_bias.at[j], 9, w_r.at[3], u_peer[j]).start()
        copy(w_x.at[0], w_x.at[j], 10, w_r.at[4], u_peer[j]).start()

    for j in (2, 4, 6):
        send_w_x(j)

    def z_own(k):
        w_z[0, k] = own_dense(k + 1)

    def z_half(h, i):
        return dense(z_links[h, i // 3, 0, i % 3], z_links[h, i // 3, 1, i % 3])

    def z_first(i):
        partial[i // 3, i % 3] = z_half(row, i)

    def z_second(i):
        w_z[i // 3, i % 3] = (partial[i // 3, i % 3] + z_half(1 - row, i)).astype(jnp.bfloat16)

    loop(0, 3, z_own)
    with jax.named_scope("zw_wait"):
        links_from(row, twin, 6, w_r.at[0]).wait_recv()
    links_from(row, twin, 8, w_r.at[2]).start()
    for j in (1, 5, 3, 7):
        send_w_x(j)
    with jax.named_scope("z_first"):
        loop(3, 3 * GROUP, z_first)
    with jax.named_scope("tw_wait"):
        many(z_bias, 7, w_r.at[1]).wait_recv()
        links_from(1 - row, twin, 8, w_r.at[2]).wait_recv()
    with jax.named_scope("z_dense"):
        loop(3, 3 * GROUP, z_second)

    def z_layers(c):
        with jax.named_scope("zin_wait"):
            many(z_in.at[c], 1, zi_r.at[c]).wait_recv()
        slots = [act0[c, z]] + [z_in[c, j] for j in range(1, GROUP)]
        slots = three_layers(slots, w_z, z_bias)
        back[c, 0] = slots[0]
        for j in range(1, GROUP):
            z_out[c, j] = slots[j]
        for j in FAR_FIRST:
            copy(z_out.at[c, j], back.at[c, j], 2, zo_r.at[c], z_peer[j]).start()

    def to_x(c):
        with jax.named_scope("zout_wait"):
            many(back.at[c], 2, zo_r.at[c]).wait_recv()
        for j in X_FAR_FIRST:
            copy(back.at[c, u_of[j]], x_in.at[c, j], 3, xi_r.at[c], u_peer[j]).start()

    def x_weights():
        with jax.named_scope("xw_wait"):
            many(x_bias, 9, w_r.at[3]).wait_recv()
            many(w_x, 10, w_r.at[4]).wait_recv()

    def x_layers(c):
        pl.when(c == 0)(x_weights)
        with jax.named_scope("xin_wait"):
            many(x_in.at[c], 3, xi_r.at[c]).wait_recv()
        slots = [back[c, u]] + [x_in[c, j] for j in range(1, GROUP)]
        slots = three_layers(slots, w_x, x_bias)
        home[c, 0] = slots[0]
        for j in range(1, GROUP):
            x_out[c, j] = slots[j]

        def to_both():
            for j in X_FAR_FIRST:
                copy(x_out.at[c, j], home.at[c, j], 4, xo_r.at[c], u_peer[j]).start()
                copy(x_out.at[c, j], partner_home.at[c, j], 5, pl_r.at[c], other[j]).start()
            copy(home.at[c, 0], partner_home.at[c, 0], 5, pl_r.at[c], partner).start()

        def to_one():
            for j in X_FAR_FIRST:
                copy(x_out.at[c, j], home.at[c, j], 4, xo_r.at[c], u_peer[j]).start()

        pl.when(c >= chunks - BOTH)(to_both)
        pl.when(c < chunks - BOTH)(to_one)

    def last_copy(c):
        return copy(home.at[c], partner_home.at[c], 5, pl_r.at[c], partner)

    def to_partner(c):
        with jax.named_scope("xout_wait"):
            many(home.at[c], 4, xo_r.at[c]).wait_recv()
        pl.when(c < chunks - BOTH)(lambda: last_copy(c).start())

    def last(c):
        with jax.named_scope("pl_wait"):
            last_copy(c).wait_recv()
        for j in range(GROUP):
            preact = end_layer(home[c, j], partner_home[c, j], 1, LAYERS - 1)
            at = xor(zb, [(ub[k] + ((j >> k) & 1)) % 2 for k in range(3)])
            out[c, at] = jnp.minimum(preact, CEILING).astype(jnp.bfloat16)
        pltpu.make_async_copy(out.at[c], out_hbm.at[c], local.at[4]).start()

    def steady(i, _):
        pl.when(i < chunks)(lambda: z_layers(i))
        for stage, lag in zip((to_x, x_layers, to_partner, last), LAGS):
            pl.when((i >= lag) & (i < chunks + lag))(functools.partial(stage, i - lag))
        return 0

    lax.fori_loop(0, chunks + LAGS[-1], steady, 0)

    with jax.named_scope("drain"):
        for at, ref in (
            (0, features),
            (1, z_in.at[:, 1:GROUP]),
            (2, z_out.at[:, 1:GROUP]),
            (3, x_in.at[:, 1:GROUP]),
            (4, x_out.at[:, 1:GROUP]),
            (5, home),
            (6, z_links.at[0, 1:GROUP]),
            (7, z_bias.at[1:GROUP]),
            (8, z_links.at[0, 1:GROUP]),
            (9, x_bias.at[1:GROUP]),
            (10, w_x.at[1:GROUP]),
        ):
            copy(ref, ref, at, w_r.at[0], partner).wait_send()
        pltpu.make_async_copy(out, out_hbm, local.at[4]).wait()


def finish_kernel(source, result, before, after, arrived, stored):
    loads = [pltpu.make_async_copy(source.at[k], before.at[k], arrived.at[k]) for k in range(PARTS)]
    stores = [pltpu.make_async_copy(after.at[k], result.at[k], stored.at[k]) for k in range(PARTS)]
    for one in loads:
        one.start()
    for k in range(PARTS):
        loads[k].wait()
        after[k] = jnp.maximum(before[k], 0)
        stores[k].start()
    for one in stores:
        one.wait()


def shards(features, link_values, link_columns, layer_bias):
    rows, width = features.shape
    piece = rows // (CHUNKS * GROUP)
    tiled = (CHUNKS, GROUP, piece, width)
    layers, fan_in, _ = link_values.shape
    hbm = pl.BlockSpec(memory_space=pltpu.HBM)
    act = pltpu.VMEM(tiled, jnp.bfloat16)
    biases = pltpu.VMEM((GROUP, 3, 1, width), jnp.float32)
    wide = pltpu.VMEM((GROUP, 3, 2 * width, width), jnp.bfloat16)
    out = pl.pallas_call(
        kernel,
        out_shape=jax.ShapeDtypeStruct(tiled, jnp.bfloat16),
        in_specs=[hbm] * 4,
        out_specs=hbm,
        scratch_shapes=[
            act,
            pltpu.VMEM(link_values.shape, jnp.bfloat16),
            pltpu.VMEM(link_columns.shape, jnp.int32),
            pltpu.VMEM(layer_bias.shape, jnp.float32),
        ]
        + [act] * 10
        + [
            pltpu.VMEM((GROUP, 3, 2 * width, width), jnp.float32),
            pltpu.VMEM((2, GROUP, 2, 3, fan_in // 2, width), jnp.bfloat16),
            biases,
            biases,
            pltpu.VMEM((2, 2 * width, width), jnp.bfloat16),
            wide,
            wide,
            pltpu.SemaphoreType.DMA((11,)),
        ]
        + [pltpu.SemaphoreType.DMA((CHUNKS,))] * 6
        + [pltpu.SemaphoreType.DMA((5,))] * 2,
        compiler_params=pltpu.CompilerParams(
            collective_id=0, has_side_effects=True, vmem_limit_bytes=VMEM_LIMIT
        ),
    )(features.reshape(tiled), link_values, link_columns, layer_bias)
    parts = (PARTS, rows // PARTS, width)
    result = pl.pallas_call(
        finish_kernel,
        out_shape=jax.ShapeDtypeStruct(parts, jnp.bfloat16),
        in_specs=[hbm],
        out_specs=hbm,
        scratch_shapes=[pltpu.VMEM(parts, jnp.bfloat16)] * 2 + [pltpu.SemaphoreType.DMA((PARTS,))] * 2,
        compiler_params=pltpu.CompilerParams(vmem_limit_bytes=VMEM_LIMIT),
    )(out.reshape(parts))
    return result.reshape(rows, width)


def solution(mesh):
    return jax.shard_map(
        shards,
        mesh=mesh,
        in_specs=(P("row", "blk"), P(None, None, "blk"), P(None, None, "blk"), P(None, "blk")),
        out_specs=P("row", "blk"),
        check_vma=False,
    )
```
